32 devices in a mesh: az: 4 (over y, x), rad: 8 (over z, core).
Axes of the slice: x: 2, y: 2, z: 4, core: 2. Of those that a mesh axis runs over, the one named last changes fastest.
Arguments:
- fields: float32 [5, 96, 32, 512], P(None, 'rad', None, 'az'), may hold values from -6 to 6
- shift: int32 [96], replicated, may hold values from 0 to 511
- fraction: float32 [96], replicated, may hold values from -0.5 to 0.5
- radial_rate: float32 [96, 32], replicated, may hold values from -0.4 to 0.4
Outputs:
- updated: float32 [5, 96, 32, 512], P(None, 'rad', None, 'az')
The draws below stay inside these ranges and needn't reach their ends.
All inputs are finite; a program needn't handle non-finite values.
Results may differ from the reference program's by a relative error of at most 0.0003.
Values sent between devices are 32-bit elements; how exact they have to be, the bound alone decides.
A program may use at most 64 MiB of HBM per device.

```python
import jax
import jax.numpy as jnp
from jax import lax

NP = 32
NF = 5
NA = 512
NR = 96


def touch_ends(entries, rng, low, largest):
    extent = entries.shape
    index_at = [jax.random.randint(jax.random.fold_in(rng, axis), (), 0, extent[axis]) for axis in range(len(extent))]
    entries = entries.at[tuple(index_at)].set(low)
    longest = extent.index(max(extent))
    index_at[longest] = (index_at[longest] + 1) % extent[longest]
    return entries.at[tuple(index_at)].set(largest)


def level_of(key, shape, cuts, low, high):
    level, own = 1.0, jax.random.fold_in(key, 6)
    for dim, shards_of in cuts:
        steps = jnp.exp(jax.random.uniform(jax.random.fold_in(own, dim), (shards_of,), jnp.float32, low / len(cuts), high / len(cuts)))
        level = level * jnp.repeat(steps, shape[dim] // shards_of).reshape([-1 if axis == dim else 1 for axis in range(len(shape))])
    return level


def gaussian(key, dims, scale, reach, pieces=(), kind=jnp.bfloat16):
    entries = scale * jax.random.normal(key, dims, jnp.float32)
    if pieces:
        entries = entries * level_of(key, dims, pieces, -0.22, 0.18)
    return jnp.clip(entries, -reach, reach).astype(kind)


def setup_inputs(seed: int = 0) -> dict:
    splits = jax.random.split(jax.random.key(seed), 5)
    fields = gaussian(splits[0], (NF, NR, NP, NA), 1.0, 6.0, ((1, 8), (3, 4)), jnp.float32)
    shift = touch_ends(jax.random.randint(splits[1], (NR,), 0, NA), jax.random.fold_in(splits[1], 1), 0, NA - 1).astype(jnp.int32)
    fraction = jnp.clip(jax.random.uniform(splits[2], (NR,), jnp.float32, -0.5, 0.5), -0.5, 0.5)
    radial_rate = jnp.clip(jax.random.uniform(splits[3], (NR, NP), jnp.float32, -0.4, 0.4), -0.4, 0.4)
    return {"fields": fields, "shift": shift, "fraction": fraction, "radial_rate": radial_rate}


def cut(values, low, count, axis):
    return lax.slice_in_dim(values, low, low + count, axis=axis)


def limited(left, right):
    steep = jnp.minimum(jnp.minimum(2.0 * jnp.abs(left), 2.0 * jnp.abs(right)), 0.5 * jnp.abs(left + right))
    return jnp.where(left * right > 0.0, jnp.sign(left) * steep, 0.0)


def flux_change(padded, courant, axis):
    count = padded.shape[axis] - 4
    left = cut(padded, 1, count + 2, axis) - cut(padded, 0, count + 2, axis)
    right = cut(padded, 2, count + 2, axis) - cut(padded, 1, count + 2, axis)
    slope = limited(left, right)
    forward = cut(padded, 1, count + 1, axis) + 0.5 * (1.0 - courant) * cut(slope, 0, count + 1, axis)
    backward = cut(padded, 2, count + 1, axis) - 0.5 * (1.0 + courant) * cut(slope, 1, count + 1, axis)
    flux = courant * jnp.where(courant > 0.0, forward, backward)
    return cut(flux, 1, count, axis) - cut(flux, 0, count, axis)


def one_field(single, shift, fraction, face_rates):
    rolled = lax.map(lambda item: jnp.roll(item[0], item[1], axis=-1), (single, shift))
    padded = jnp.concatenate([rolled[:, :, -2:], rolled, rolled[:, :, :2]], axis=2)
    azimuthal = rolled - flux_change(padded, fraction[:, None, None], 2)
    zeros = jnp.zeros((2,) + azimuthal.shape[1:], jnp.float32)
    radial = jnp.concatenate([zeros, azimuthal, zeros], axis=0)
    return azimuthal - flux_change(radial, face_rates[:, :, None], 0)


def reference(fields, shift, fraction, radial_rate):
    edge = jnp.zeros((1, radial_rate.shape[1]), jnp.float32)
    face_rates = jnp.concatenate([edge, radial_rate[:-1], edge], axis=0)
    return lax.map(lambda single: one_field(single, shift, fraction, face_rates), fields)
```

```python
import functools

import jax
import jax.numpy as jnp
from jax import lax
from jax.experimental import pallas as pl
from jax.experimental.pallas import tpu as pltpu
from jax.sharding import PartitionSpec as P

MESH = pl.DeviceIdType.MESH


def half_slope(left, right):
    low = jnp.maximum(jnp.minimum(left, right), 0.0)
    high = jnp.minimum(jnp.maximum(left, right), 0.0)
    return jnp.maximum(jnp.minimum(0.25 * (left + right), low), high)


def chunks_of(fields, rows, group):
    rest = rows // group - 1
    if rest == 0:
        return [(True, f, 1) for f in range(fields)]
    return [(True, 0, fields)] + [(False, f, 1) for f in range(fields)]


def kernel(
    group, rings, chunks,
    fields, shift, fraction, rates,
    out,
    own, landed, rate, bend, *rest,
):
    count = len(chunks)
    gathered, results = rest[:count], rest[count : 2 * count]
    in_sem, own_sem, send1, recv1, send2, recv2, ghost_send, ghost_recv = rest[2 * count :]
    nf, rows, polar, width = fields.shape
    me, ring = lax.axis_index("az"), lax.axis_index("rad")
    more = rows // group - 1
    start = ring * rows

    def base(first, d):
        if first:
            return jnp.where(d < 2, d, jnp.where(d < 4, rows - 4 + d, d - 2))
        return group - 2 + d * more

    def height(first):
        return 1 if first else more

    stages = [
        pltpu.make_async_copy(fields.at[:, pl.ds(0, group - 2)], own.at[:, pl.ds(0, group - 2)], in_sem.at[0]),
        pltpu.make_async_copy(fields.at[:, pl.ds(rows - 2, 2)], own.at[:, pl.ds(rows - 2, 2)], in_sem.at[1]),
    ]
    if more:
        stages.append(
            pltpu.make_async_copy(
                fields.at[:, pl.ds(group - 2, rows - group)],
                own.at[:, pl.ds(group - 2, rows - group)],
                in_sem.at[2],
            )
        )
    for copy in stages:
        copy.start()
    mine = []
    for c, (first, f0, n) in enumerate(chunks):
        copy = pltpu.make_async_copy(
            fields.at[pl.ds(f0, n), pl.ds(base(first, me), height(first))],
            gathered[c].at[me],
            own_sem.at[c],
        )
        copy.start()
        mine.append(copy)

    barrier = pltpu.get_barrier_semaphore()
    for step in range(1, group):
        pl.semaphore_signal(
            barrier, inc=1, device_id=(lax.rem(me + step, group), ring), device_id_type=MESH
        )

    @pl.when(ring > 0)
    def _():
        pl.semaphore_signal(barrier, inc=1, device_id=(me, ring - 1), device_id_type=MESH)

    @pl.when(ring < rings - 1)
    def _():
        pl.semaphore_signal(barrier, inc=1, device_id=(me, ring + 1), device_id_type=MESH)

    table = rates[...]
    place = lax.broadcasted_iota(jnp.int32, table.shape, 1)
    for j in range(rows + 1):
        column = jnp.sum(
            jnp.where(place == start - 1 + j, table, 0.0), axis=1, keepdims=True
        )
        if j == 0:
            column = jnp.where(ring > 0, column, 0.0)
        if j == rows:
            column = jnp.where(ring < rings - 1, column, 0.0)
        spread = jnp.broadcast_to(column, (polar, width))
        size = jnp.abs(spread)
        rate[j] = spread
        bend[j] = size * (1.0 - size)

    @pl.when(ring == 0)
    def _():
        landed[:, 0:2] = jnp.zeros((nf, 2, polar, width), jnp.float32)

    @pl.when(ring == rings - 1)
    def _():
        landed[:, rows + 2 : rows + 4] = jnp.zeros((nf, 2, polar, width), jnp.float32)

    neighbours = (group - 1) + jnp.where(ring > 0, 1, 0) + jnp.where(ring < rings - 1, 1, 0)
    pl.semaphore_wait(barrier, neighbours)

    def out_copy(c, d):
        first, f0, n = chunks[c]
        return pltpu.make_async_remote_copy(
            src_ref=own.at[pl.ds(f0, n), pl.ds(base(first, d), height(first))],
            dst_ref=gathered[c].at[me],
            send_sem=send1.at[c, d],
            recv_sem=recv1.at[c, me],
            device_id=(d, ring),
            device_id_type=MESH,
        )

    def in_copy(c, s):
        first, f0, n = chunks[c]
        return pltpu.make_async_remote_copy(
            src_ref=gathered[c].at[s],
            dst_ref=gathered[c].at[s],
            send_sem=send1.at[c, s],
            recv_sem=recv1.at[c, s],
            device_id=(s, ring),
            device_id_type=MESH,
        )

    def back_copy(c, d):
        first, f0, n = chunks[c]
        return pltpu.make_async_remote_copy(
            src_ref=results[c].at[d],
            dst_ref=landed.at[pl.ds(f0, n), pl.ds(2 + base(first, me), height(first))],
            send_sem=send2.at[c, d],
            recv_sem=recv2.at[c, me],
            device_id=(d, ring),
            device_id_type=MESH,
        )

    def home_copy(c, s):
        first, f0, n = chunks[c]
        target = landed.at[pl.ds(f0, n), pl.ds(2 + base(first, s), height(first))]
        return pltpu.make_async_remote_copy(
            src_ref=target,
            dst_ref=target,
            send_sem=send2.at[c, s],
            recv_sem=recv2.at[c, s],
            device_id=(s, ring),
            device_id_type=MESH,
        )

    def peers():
        return [lax.rem(me + step, group) for step in range(1, group)]

    for c in range(count):
        if c == 0:
            stages[0].wait()
            stages[1].wait()
        if c == 1 and more:
            stages[2].wait()
        for d in peers():
            out_copy(c, d).start()

    lane = lax.broadcasted_iota(jnp.int32, (polar, width), 1)
    at_first, at_last = lane == 0, lane == width - 1

    def previous(blocks):
        turned = [pltpu.roll(b, 1, 1) for b in blocks]
        return [jnp.where(at_first, turned[p - 1], turned[p]) for p in range(group)]

    def following(blocks):
        turned = [pltpu.roll(b, width - 1, 1) for b in blocks]
        return [jnp.where(at_last, turned[(p + 1) % group], turned[p]) for p in range(group)]

    cycle = group * width

    def azimuth(c):
        first, f0, n = chunks[c]
        source, target = gathered[c], results[c]
        for k in range(height(first)):
            row = start + base(first, me) + k
            courant = fraction[row]
            ahead = courant > 0.0
            amount = shift[row] + jnp.where(ahead, cycle, cycle - 1)
            whole = lax.rem(amount // width, group)
            part = lax.rem(amount, width)
            size = jnp.abs(courant)
            bent = size * (1.0 - size)
            beyond = lane >= part

            for f in range(n):
                turned = [
                    pltpu.roll(source[lax.rem(p + group - whole, group), f, k], part, 1)
                    for p in range(group)
                ]
                q = [jnp.where(beyond, turned[p], turned[p - 1]) for p in range(group)]
                before = previous(q)
                left = [x - y for x, y in zip(q, before)]
                right = following(left)
                value = [
                    courant * x + bent * half_slope(l, r) for x, l, r in zip(q, left, right)
                ]
                lower = previous(value)
                for p in range(group):
                    kept = jnp.where(ahead, q[p], before[p])
                    target[p, f, k] = kept - (value[p] - lower[p])
        landed[pl.ds(f0, n), pl.ds(2 + base(first, me), height(first))] = target[me]

    ghosts = [
        pltpu.make_async_remote_copy(
            src_ref=landed.at[:, pl.ds(2, 2)],
            dst_ref=landed.at[:, pl.ds(rows + 2, 2)],
            send_sem=ghost_send.at[0],
            recv_sem=ghost_recv.at[0],
            device_id=(me, jnp.maximum(ring - 1, 0)),
            device_id_type=MESH,
        ),
        pltpu.make_async_remote_copy(
            src_ref=landed.at[:, pl.ds(rows, 2)],
            dst_ref=landed.at[:, pl.ds(0, 2)],
            send_sem=ghost_send.at[1],
            recv_sem=ghost_recv.at[1],
            device_id=(me, jnp.minimum(ring + 1, rings - 1)),
            device_id_type=MESH,
        ),
    ]

    def radial(f):
        def cell(i):
            return landed[f, i]

        q1, q2 = cell(1), cell(2)
        d1 = q1 - cell(0)
        d2 = q2 - q1
        h1 = half_slope(d1, d2)
        below = None
        for j in range(rows + 1):
            q3 = cell(j + 3)
            d3 = q3 - q2
            h2 = half_slope(d2, d3)
            c, b = rate[j], bend[j]
            ahead = c > 0.0
            flux = c * jnp.where(ahead, q1, q2) + b * jnp.where(ahead, h1, h2)
            if j > 0:
                out[f, j - 1] = q1 - (flux - below)
            below = flux
            q1, q2, d2, h1 = q2, q3, d3, h2

    edges = 1 if more else count

    for c in range(count):
        mine[c].wait()
        for s in peers():
            in_copy(c, s).wait_recv()
        azimuth(c)
        for d in peers():
            back_copy(c, d).start()

    for c in range(edges):
        for s in peers():
            home_copy(c, s).wait_recv()

    @pl.when(ring > 0)
    def _():
        ghosts[0].start()

    @pl.when(ring < rings - 1)
    def _():
        ghosts[1].start()

    @pl.when(ring > 0)
    def _():
        ghosts[1].wait_recv()

    @pl.when(ring < rings - 1)
    def _():
        ghosts[0].wait_recv()

    for f in range(nf):
        if more:
            for s in peers():
                home_copy(edges + f, s).wait_recv()
        radial(f)

    for c in range(count):
        for d in peers():
            out_copy(c, d).wait_send()
            back_copy(c, d).wait_send()

    @pl.when(ring > 0)
    def _():
        ghosts[0].wait_send()

    @pl.when(ring < rings - 1)
    def _():
        ghosts[1].wait_send()


def shards(fields, shift, fraction, radial_rate):
    nf, rows, polar, width = fields.shape
    group, rings = lax.axis_size("az"), lax.axis_size("rad")
    chunks = chunks_of(nf, rows, group)
    more = rows // group - 1
    boxes = [
        pltpu.VMEM((group, n, 1 if first else more, polar, width), jnp.float32)
        for first, f0, n in chunks
    ]
    count = len(chunks)
    dma = pltpu.SemaphoreType.DMA
    return pl.pallas_call(
        functools.partial(kernel, group, rings, chunks),
        out_shape=jax.ShapeDtypeStruct(fields.shape, jnp.float32),
        in_specs=[
            pl.BlockSpec(memory_space=pltpu.HBM),
            pl.BlockSpec(memory_space=pltpu.SMEM),
            pl.BlockSpec(memory_space=pltpu.SMEM),
            pl.BlockSpec(memory_space=pltpu.VMEM),
        ],
        out_specs=pl.BlockSpec(memory_space=pltpu.VMEM),
        scratch_shapes=[
            pltpu.VMEM((nf, rows, polar, width), jnp.float32),
            pltpu.VMEM((nf, rows + 4, polar, width), jnp.float32),
            pltpu.VMEM((rows + 1, polar, width), jnp.float32),
            pltpu.VMEM((rows + 1, polar, width), jnp.float32),
            *boxes,
            *boxes,
            dma((3,)),
            dma((count,)),
            dma((count, group)),
            dma((count, group)),
            dma((count, group)),
            dma((count, group)),
            dma((2,)),
            dma((2,)),
        ],
        compiler_params=pltpu.CompilerParams(collective_id=0, has_side_effects=True),
    )(fields, shift, fraction, radial_rate.T)


def solution(mesh):
    placed = (P(None, "rad", None, "az"), P(), P(), P())
    return jax.shard_map(
        shards, mesh=mesh, in_specs=placed, out_specs=P(None, "rad", None, "az"), check_vma=False
    )
```

```python
import functools

import jax
import jax.numpy as jnp
from jax import lax
from jax.experimental import pallas as pl
from jax.experimental.pallas import tpu as pltpu
from jax.sharding import PartitionSpec as P

MESH = pl.DeviceIdType.MESH


def half_slope(left, right):
    low = jnp.maximum(jnp.minimum(left, right), 0.0)
    high = jnp.minimum(jnp.maximum(left, right), 0.0)
    return jnp.maximum(jnp.minimum(0.25 * (left + right), low), high)


def chunks_of(fields, rows, group):
    rest = rows // group - 1
    if rest == 0:
        return [(True, f, 1) for f in range(fields)]
    return [(True, 0, fields)] + [(False, f, 1) for f in range(fields)]


def kernel(
    group, rings, chunks,
    fields, shift_in, fraction_in, rates_in,
    out,
    own, landed, rate, bend, shift, fraction, rates, *rest,
):
    count = len(chunks)
    gathered, results = rest[:count], rest[count : 2 * count]
    small_sem, in_sem, own_sem, send1, recv1, send2, recv2, ghost_send, ghost_recv = rest[2 * count :]
    nf, rows, polar, width = fields.shape
    me, ring = lax.axis_index("az"), lax.axis_index("rad")
    more = rows // group - 1
    start = ring * rows

    def base(first, d):
        if first:
            return jnp.where(d < 2, d, jnp.where(d < 4, rows - 4 + d, d - 2))
        return group - 2 + d * more

    def height(first):
        return 1 if first else more

    small = [
        pltpu.make_async_copy(rates_in, rates, small_sem.at[0]),
        pltpu.make_async_copy(shift_in, shift, small_sem.at[1]),
        pltpu.make_async_copy(fraction_in, fraction, small_sem.at[2]),
    ]
    for copy in small:
        copy.start()

    stages = [
        pltpu.make_async_copy(fields.at[:, pl.ds(0, group - 2)], own.at[:, pl.ds(0, group - 2)], in_sem.at[0]),
        pltpu.make_async_copy(fields.at[:, pl.ds(rows - 2, 2)], own.at[:, pl.ds(rows - 2, 2)], in_sem.at[1]),
    ]
    if more:
        stages.append(
            pltpu.make_async_copy(
                fields.at[:, pl.ds(group - 2, rows - group)],
                own.at[:, pl.ds(group - 2, rows - group)],
                in_sem.at[2],
            )
        )
    for copy in stages:
        copy.start()
    mine = []
    for c, (first, f0, n) in enumerate(chunks):
        copy = pltpu.make_async_copy(
            fields.at[pl.ds(f0, n), pl.ds(base(first, me), height(first))],
            gathered[c].at[me],
            own_sem.at[c],
        )
        copy.start()
        mine.append(copy)

    barrier = pltpu.get_barrier_semaphore()
    for step in range(1, group):
        pl.semaphore_signal(
            barrier, inc=1, device_id=(lax.rem(me + step, group), ring), device_id_type=MESH
        )

    @pl.when(ring > 0)
    def _():
        pl.semaphore_signal(barrier, inc=1, device_id=(me, ring - 1), device_id_type=MESH)

    @pl.when(ring < rings - 1)
    def _():
        pl.semaphore_signal(barrier, inc=1, device_id=(me, ring + 1), device_id_type=MESH)

    small[0].wait()
    table = rates[...]
    place = lax.broadcasted_iota(jnp.int32, table.shape, 1)
    for j in range(rows + 1):
        column = jnp.sum(
            jnp.where(place == start - 1 + j, table, 0.0), axis=1, keepdims=True
        )
        if j == 0:
            column = jnp.where(ring > 0, column, 0.0)
        if j == rows:
            column = jnp.where(ring < rings - 1, column, 0.0)
        spread = jnp.broadcast_to(column, (polar, width))
        size = jnp.abs(spread)
        rate[j] = spread
        bend[j] = size * (1.0 - size)

    @pl.when(ring == 0)
    def _():
        landed[:, 0:2] = jnp.zeros((nf, 2, polar, width), jnp.float32)

    @pl.when(ring == rings - 1)
    def _():
        landed[:, rows + 2 : rows + 4] = jnp.zeros((nf, 2, polar, width), jnp.float32)

    neighbours = (group - 1) + jnp.where(ring > 0, 1, 0) + jnp.where(ring < rings - 1, 1, 0)
    pl.semaphore_wait(barrier, neighbours)

    def out_copy(c, d):
        first, f0, n = chunks[c]
        return pltpu.make_async_remote_copy(
            src_ref=own.at[pl.ds(f0, n), pl.ds(base(first, d), height(first))],
            dst_ref=gathered[c].at[me],
            send_sem=send1.at[c, d],
            recv_sem=recv1.at[c, me],
            device_id=(d, ring),
            device_id_type=MESH,
        )

    def in_copy(c, s):
        first, f0, n = chunks[c]
        return pltpu.make_async_remote_copy(
            src_ref=gathered[c].at[s],
            dst_ref=gathered[c].at[s],
            send_sem=send1.at[c, s],
            recv_sem=recv1.at[c, s],
            device_id=(s, ring),
            device_id_type=MESH,
        )

    def back_copy(c, d):
        first, f0, n = chunks[c]
        return pltpu.make_async_remote_copy(
            src_ref=results[c].at[d],
            dst_ref=landed.at[pl.ds(f0, n), pl.ds(2 + base(first, me), height(first))],
            send_sem=send2.at[c, d],
            recv_sem=recv2.at[c, me],
            device_id=(d, ring),
            device_id_type=MESH,
        )

    def home_copy(c, s):
        first, f0, n = chunks[c]
        target = landed.at[pl.ds(f0, n), pl.ds(2 + base(first, s), height(first))]
        return pltpu.make_async_remote_copy(
            src_ref=target,
            dst_ref=target,
            send_sem=send2.at[c, s],
            recv_sem=recv2.at[c, s],
            device_id=(s, ring),
            device_id_type=MESH,
        )

    def peers():
        return [lax.rem(me + step, group) for step in range(1, group)]

    for c in range(count):
        if c == 0:
            stages[0].wait()
            stages[1].wait()
        if c == 1 and more:
            stages[2].wait()
        for d in peers():
            out_copy(c, d).start()

    lane = lax.broadcasted_iota(jnp.int32, (polar, width), 1)
    at_first, at_last = lane == 0, lane == width - 1

    def previous(blocks):
        turned = [pltpu.roll(b, 1, 1) for b in blocks]
        return [jnp.where(at_first, turned[p - 1], turned[p]) for p in range(group)]

    def following(blocks):
        turned = [pltpu.roll(b, width - 1, 1) for b in blocks]
        return [jnp.where(at_last, turned[(p + 1) % group], turned[p]) for p in range(group)]

    cycle = group * width

    def azimuth(c):
        first, f0, n = chunks[c]
        source, target = gathered[c], results[c]
        for k in range(height(first)):
            row = start + base(first, me) + k
            courant = fraction[row]
            ahead = courant > 0.0
            amount = shift[row] + jnp.where(ahead, cycle, cycle - 1)
            whole = lax.rem(amount // width, group)
            part = lax.rem(amount, width)
            size = jnp.abs(courant)
            bent = size * (1.0 - size)
            beyond = lane >= part

            for f in range(n):
                turned = [
                    pltpu.roll(source[lax.rem(p + group - whole, group), f, k], part, 1)
                    for p in range(group)
                ]
                q = [jnp.where(beyond, turned[p], turned[p - 1]) for p in range(group)]
                before = previous(q)
                left = [x - y for x, y in zip(q, before)]
                right = following(left)
                value = [
                    courant * x + bent * half_slope(l, r) for x, l, r in zip(q, left, right)
                ]
                lower = previous(value)
                for p in range(group):
                    kept = jnp.where(ahead, q[p], before[p])
                    target[p, f, k] = kept - (value[p] - lower[p])
        landed[pl.ds(f0, n), pl.ds(2 + base(first, me), height(first))] = target[me]

    ghosts = [
        pltpu.make_async_remote_copy(
            src_ref=landed.at[:, pl.ds(2, 2)],
            dst_ref=landed.at[:, pl.ds(rows + 2, 2)],
            send_sem=ghost_send.at[0],
            recv_sem=ghost_recv.at[0],
            device_id=(me, jnp.maximum(ring - 1, 0)),
            device_id_type=MESH,
        ),
        pltpu.make_async_remote_copy(
            src_ref=landed.at[:, pl.ds(rows, 2)],
            dst_ref=landed.at[:, pl.ds(0, 2)],
            send_sem=ghost_send.at[1],
            recv_sem=ghost_recv.at[1],
            device_id=(me, jnp.minimum(ring + 1, rings - 1)),
            device_id_type=MESH,
        ),
    ]

    def radial(f):
        def cell(i):
            return landed[f, i]

        q1, q2 = cell(1), cell(2)
        d1 = q1 - cell(0)
        d2 = q2 - q1
        h1 = half_slope(d1, d2)
        below = None
        for j in range(rows + 1):
            q3 = cell(j + 3)
            d3 = q3 - q2
            h2 = half_slope(d2, d3)
            c, b = rate[j], bend[j]
            ahead = c > 0.0
            flux = c * jnp.where(ahead, q1, q2) + b * jnp.where(ahead, h1, h2)
            if j > 0:
                out[f, j - 1] = q1 - (flux - below)
            below = flux
            q1, q2, d2, h1 = q2, q3, d3, h2

    edges = 1 if more else count

    small[1].wait()
    small[2].wait()
    for c in range(count):
        mine[c].wait()
        for s in peers():
            in_copy(c, s).wait_recv()
        azimuth(c)
        for d in peers():
            back_copy(c, d).start()

    for c in range(edges):
        for s in peers():
            home_copy(c, s).wait_recv()

    @pl.when(ring > 0)
    def _():
        ghosts[0].start()

    @pl.when(ring < rings - 1)
    def _():
        ghosts[1].start()

    @pl.when(ring > 0)
    def _():
        ghosts[1].wait_recv()

    @pl.when(ring < rings - 1)
    def _():
        ghosts[0].wait_recv()

    for f in range(nf):
        if more:
            for s in peers():
                home_copy(edges + f, s).wait_recv()
        radial(f)

    for c in range(count):
        for d in peers():
            out_copy(c, d).wait_send()
            back_copy(c, d).wait_send()

    @pl.when(ring > 0)
    def _():
        ghosts[0].wait_send()

    @pl.when(ring < rings - 1)
    def _():
        ghosts[1].wait_send()


def shards(fields, shift, fraction, radial_rate):
    nf, rows, polar, width = fields.shape
    group, rings = lax.axis_size("az"), lax.axis_size("rad")
    chunks = chunks_of(nf, rows, group)
    more = rows // group - 1
    boxes = [
        pltpu.VMEM((group, n, 1 if first else more, polar, width), jnp.float32)
        for first, f0, n in chunks
    ]
    count = len(chunks)
    dma = pltpu.SemaphoreType.DMA
    operands = (fields, shift, fraction, radial_rate.T)
    return pl.pallas_call(
        functools.partial(kernel, group, rings, chunks),
        out_shape=jax.ShapeDtypeStruct(fields.shape, jnp.float32),
        in_specs=[pl.BlockSpec(memory_space=pltpu.HBM)] * 4,
        out_specs=pl.BlockSpec(memory_space=pltpu.VMEM),
        scratch_shapes=[
            pltpu.VMEM((nf, rows, polar, width), jnp.float32),
            pltpu.VMEM((nf, rows + 4, polar, width), jnp.float32),
            pltpu.VMEM((rows + 1, polar, width), jnp.float32),
            pltpu.VMEM((rows + 1, polar, width), jnp.float32),
            pltpu.SMEM(shift.shape, jnp.int32),
            pltpu.SMEM(fraction.shape, jnp.float32),
            pltpu.VMEM(radial_rate.shape[::-1], jnp.float32),
            *boxes,
            *boxes,
            dma((3,)),
            dma((3,)),
            dma((count,)),
            dma((count, group)),
            dma((count, group)),
            dma((count, group)),
            dma((count, group)),
            dma((2,)),
            dma((2,)),
        ],
        compiler_params=pltpu.CompilerParams(
            collective_id=0, has_side_effects=True, vmem_limit_bytes=10 * fields.size * 4
        ),
    )(*(pltpu.with_memory_space_constraint(x, pltpu.HBM) for x in operands))


def solution(mesh):
    placed = (P(None, "rad", None, "az"), P(), P(), P())
    return jax.shard_map(
        shards, mesh=mesh, in_specs=placed, out_specs=P(None, "rad", None, "az"), check_vma=False
    )
```

```python
import functools

import jax
import jax.numpy as jnp
from jax import lax
from jax.experimental import pallas as pl
from jax.experimental.pallas import tpu as pltpu
from jax.sharding import PartitionSpec as P

MESH = pl.DeviceIdType.MESH


def half_slope(left, right):
    low = jnp.maximum(jnp.minimum(left, right), 0.0)
    high = jnp.minimum(jnp.maximum(left, right), 0.0)
    return jnp.maximum(jnp.minimum(0.25 * (left + right), low), high)


def chunks_of(fields, rows, group):
    rest = rows // group - 1
    if rest == 0:
        return [(True, f, 1) for f in range(fields)]
    return [(True, 0, fields)] + [(False, f, 1) for f in range(fields)]


def peers_of(group, me):
    if group == 4:
        inner = me + 1 - 2 * lax.rem(me, 2)
        outer = lax.rem(me + 2, 4)
        return [inner, outer], [inner + outer - me]
    return [lax.rem(me + step, group) for step in range(1, group)], []


def kernel(
    group, rings, chunks,
    fields, shift_in, fraction_in, rates_in,
    out,
    own, landed, rate, bend, shift, fraction, rates, *rest,
):
    count = len(chunks)
    gathered, results = rest[:count], rest[count : 2 * count]
    small_sem, in_sem, own_sem, send1, recv1, send2, recv2, ghost_send, ghost_recv, passed = rest[2 * count :]
    nf, rows, polar, width = fields.shape
    me, ring = lax.axis_index("az"), lax.axis_index("rad")
    more = rows // group - 1
    start = ring * rows

    def base(first, d):
        if first:
            return jnp.where(d < 2, d, jnp.where(d < 4, rows - 4 + d, d - 2))
        return group - 2 + d * more

    def height(first):
        return 1 if first else more

    near, far = peers_of(group, me)
    barrier = pltpu.get_barrier_semaphore()
    for d in near:
        pl.semaphore_signal(barrier, inc=1, device_id=(d, ring), device_id_type=MESH)

    @pl.when(ring > 0)
    def _():
        pl.semaphore_signal(barrier, inc=1, device_id=(me, ring - 1), device_id_type=MESH)

    @pl.when(ring < rings - 1)
    def _():
        pl.semaphore_signal(barrier, inc=1, device_id=(me, ring + 1), device_id_type=MESH)

    stages = [
        pltpu.make_async_copy(fields.at[:, pl.ds(0, group - 2)], own.at[:, pl.ds(0, group - 2)], in_sem.at[0]),
        pltpu.make_async_copy(fields.at[:, pl.ds(rows - 2, 2)], own.at[:, pl.ds(rows - 2, 2)], in_sem.at[1]),
    ]
    if more:
        stages.append(
            pltpu.make_async_copy(
                fields.at[:, pl.ds(group - 2, rows - group)],
                own.at[:, pl.ds(group - 2, rows - group)],
                in_sem.at[2],
            )
        )
    for copy in stages:
        copy.start()
    mine = []
    for c, (first, f0, n) in enumerate(chunks):
        copy = pltpu.make_async_copy(
            fields.at[pl.ds(f0, n), pl.ds(base(first, me), height(first))],
            gathered[c].at[me],
            own_sem.at[c],
        )
        copy.start()
        mine.append(copy)

    small = [
        pltpu.make_async_copy(rates_in, rates, small_sem.at[0]),
        pltpu.make_async_copy(shift_in, shift, small_sem.at[1]),
        pltpu.make_async_copy(fraction_in, fraction, small_sem.at[2]),
    ]
    for copy in small:
        copy.start()

    neighbours = len(near) + jnp.where(ring > 0, 1, 0) + jnp.where(ring < rings - 1, 1, 0)
    pl.semaphore_wait(barrier, neighbours)
    if far:
        pl.semaphore_signal(passed, inc=1, device_id=(near[0], ring), device_id_type=MESH)

    def out_copy(c, d):
        first, f0, n = chunks[c]
        return pltpu.make_async_remote_copy(
            src_ref=own.at[pl.ds(f0, n), pl.ds(base(first, d), height(first))],
            dst_ref=gathered[c].at[me],
            send_sem=send1.at[c, d],
            recv_sem=recv1.at[c, me],
            device_id=(d, ring),
            device_id_type=MESH,
        )

    def in_copy(c, s):
        first, f0, n = chunks[c]
        return pltpu.make_async_remote_copy(
            src_ref=gathered[c].at[s],
            dst_ref=gathered[c].at[s],
            send_sem=send1.at[c, s],
            recv_sem=recv1.at[c, s],
            device_id=(s, ring),
            device_id_type=MESH,
        )

    def back_copy(c, d):
        first, f0, n = chunks[c]
        return pltpu.make_async_remote_copy(
            src_ref=results[c].at[d],
            dst_ref=landed.at[pl.ds(f0, n), pl.ds(2 + base(first, me), height(first))],
            send_sem=send2.at[c, d],
            recv_sem=recv2.at[c, me],
            device_id=(d, ring),
            device_id_type=MESH,
        )

    def home_copy(c, s):
        first, f0, n = chunks[c]
        target = landed.at[pl.ds(f0, n), pl.ds(2 + base(first, s), height(first))]
        return pltpu.make_async_remote_copy(
            src_ref=target,
            dst_ref=target,
            send_sem=send2.at[c, s],
            recv_sem=recv2.at[c, s],
            device_id=(s, ring),
            device_id_type=MESH,
        )

    def peers():
        return far + near

    for c in range(count):
        if c == 0:
            stages[0].wait()
            stages[1].wait()
        if c == 1 and more:
            stages[2].wait()
        for d in near:
            out_copy(c, d).start()
        if c == 0 and far:
            pl.semaphore_wait(passed, 1)
        for d in far:
            out_copy(c, d).start()

    small[0].wait()
    table = rates[...]
    place = lax.broadcasted_iota(jnp.int32, table.shape, 1)
    for j in range(rows + 1):
        column = jnp.sum(
            jnp.where(place == start - 1 + j, table, 0.0), axis=1, keepdims=True
        )
        if j == 0:
            column = jnp.where(ring > 0, column, 0.0)
        if j == rows:
            column = jnp.where(ring < rings - 1, column, 0.0)
        spread = jnp.broadcast_to(column, (polar, width))
        size = jnp.abs(spread)
        rate[j] = spread
        bend[j] = size * (1.0 - size)

    @pl.when(ring == 0)
    def _():
        landed[:, 0:2] = jnp.zeros((nf, 2, polar, width), jnp.float32)

    @pl.when(ring == rings - 1)
    def _():
        landed[:, rows + 2 : rows + 4] = jnp.zeros((nf, 2, polar, width), jnp.float32)

    lane = lax.broadcasted_iota(jnp.int32, (polar, width), 1)
    at_first, at_last = lane == 0, lane == width - 1

    def previous(blocks):
        turned = [pltpu.roll(b, 1, 1) for b in blocks]
        return [jnp.where(at_first, turned[p - 1], turned[p]) for p in range(group)]

    def following(blocks):
        turned = [pltpu.roll(b, width - 1, 1) for b in blocks]
        return [jnp.where(at_last, turned[(p + 1) % group], turned[p]) for p in range(group)]

    cycle = group * width

    def azimuth(c):
        first, f0, n = chunks[c]
        source, target = gathered[c], results[c]
        for k in range(height(first)):
            row = start + base(first, me) + k
            courant = fraction[row]
            ahead = courant > 0.0
            amount = shift[row] + jnp.where(ahead, cycle, cycle - 1)
            whole = lax.rem(amount // width, group)
            part = lax.rem(amount, width)
            size = jnp.abs(courant)
            bent = size * (1.0 - size)
            beyond = lane >= part

            for f in range(n):
                turned = [
                    pltpu.roll(source[lax.rem(p + group - whole, group), f, k], part, 1)
                    for p in range(group)
                ]
                q = [jnp.where(beyond, turned[p], turned[p - 1]) for p in range(group)]
                before = previous(q)
                left = [x - y for x, y in zip(q, before)]
                right = following(left)
                value = [
                    courant * x + bent * half_slope(l, r) for x, l, r in zip(q, left, right)
                ]
                lower = previous(value)
                for p in range(group):
                    kept = jnp.where(ahead, q[p], before[p])
                    target[p, f, k] = kept - (value[p] - lower[p])
        landed[pl.ds(f0, n), pl.ds(2 + base(first, me), height(first))] = target[me]

    ghosts = [
        pltpu.make_async_remote_copy(
            src_ref=landed.at[:, pl.ds(2, 2)],
            dst_ref=landed.at[:, pl.ds(rows + 2, 2)],
            send_sem=ghost_send.at[0],
            recv_sem=ghost_recv.at[0],
            device_id=(me, jnp.maximum(ring - 1, 0)),
            device_id_type=MESH,
        ),
        pltpu.make_async_remote_copy(
            src_ref=landed.at[:, pl.ds(rows, 2)],
            dst_ref=landed.at[:, pl.ds(0, 2)],
            send_sem=ghost_send.at[1],
            recv_sem=ghost_recv.at[1],
            device_id=(me, jnp.minimum(ring + 1, rings - 1)),
            device_id_type=MESH,
        ),
    ]

    def radial(f):
        def cell(i):
            return landed[f, i]

        q1, q2 = cell(1), cell(2)
        d1 = q1 - cell(0)
        d2 = q2 - q1
        h1 = half_slope(d1, d2)
        below = None
        for j in range(rows + 1):
            q3 = cell(j + 3)
            d3 = q3 - q2
            h2 = half_slope(d2, d3)
            c, b = rate[j], bend[j]
            ahead = c > 0.0
            flux = c * jnp.where(ahead, q1, q2) + b * jnp.where(ahead, h1, h2)
            if j > 0:
                out[f, j - 1] = q1 - (flux - below)
            below = flux
            q1, q2, d2, h1 = q2, q3, d3, h2

    edges = 1 if more else count

    small[1].wait()
    small[2].wait()
    for c in range(count):
        mine[c].wait()
        for s in peers():
            in_copy(c, s).wait_recv()
        azimuth(c)
        for d in peers():
            back_copy(c, d).start()

    for c in range(edges):
        for s in peers():
            home_copy(c, s).wait_recv()

    @pl.when(ring > 0)
    def _():
        ghosts[0].start()

    @pl.when(ring < rings - 1)
    def _():
        ghosts[1].start()

    @pl.when(ring > 0)
    def _():
        ghosts[1].wait_recv()

    @pl.when(ring < rings - 1)
    def _():
        ghosts[0].wait_recv()

    for f in range(nf):
        if more:
            for s in peers():
                home_copy(edges + f, s).wait_recv()
        radial(f)

    for c in range(count):
        for d in peers():
            out_copy(c, d).wait_send()
            back_copy(c, d).wait_send()

    @pl.when(ring > 0)
    def _():
        ghosts[0].wait_send()

    @pl.when(ring < rings - 1)
    def _():
        ghosts[1].wait_send()


def shards(fields, shift, fraction, radial_rate):
    nf, rows, polar, width = fields.shape
    group, rings = lax.axis_size("az"), lax.axis_size("rad")
    chunks = chunks_of(nf, rows, group)
    more = rows // group - 1
    boxes = [
        pltpu.VMEM((group, n, 1 if first else more, polar, width), jnp.float32)
        for first, f0, n in chunks
    ]
    count = len(chunks)
    dma = pltpu.SemaphoreType.DMA
    operands = (fields, shift, fraction, radial_rate.T)
    return pl.pallas_call(
        functools.partial(kernel, group, rings, chunks),
        out_shape=jax.ShapeDtypeStruct(fields.shape, jnp.float32),
        in_specs=[pl.BlockSpec(memory_space=pltpu.HBM)] * 4,
        out_specs=pl.BlockSpec(memory_space=pltpu.VMEM),
        scratch_shapes=[
            pltpu.VMEM((nf, rows, polar, width), jnp.float32),
            pltpu.VMEM((nf, rows + 4, polar, width), jnp.float32),
            pltpu.VMEM((rows + 1, polar, width), jnp.float32),
            pltpu.VMEM((rows + 1, polar, width), jnp.float32),
            pltpu.SMEM(shift.shape, jnp.int32),
            pltpu.SMEM(fraction.shape, jnp.float32),
            pltpu.VMEM(radial_rate.shape[::-1], jnp.float32),
            *boxes,
            *boxes,
            dma((3,)),
            dma((3,)),
            dma((count,)),
            dma((count, group)),
            dma((count, group)),
            dma((count, group)),
            dma((count, group)),
            dma((2,)),
            dma((2,)),
            pltpu.SemaphoreType.REGULAR,
        ],
        compiler_params=pltpu.CompilerParams(
            collective_id=0, has_side_effects=True, vmem_limit_bytes=10 * fields.size * 4
        ),
    )(*(pltpu.with_memory_space_constraint(x, pltpu.HBM) for x in operands))


def solution(mesh):
    placed = (P(None, "rad", None, "az"), P(), P(), P())
    return jax.shard_map(
        shards, mesh=mesh, in_specs=placed, out_specs=P(None, "rad", None, "az"), check_vma=False
    )
```

```python
import functools

import jax
import jax.numpy as jnp
from jax import lax
from jax.experimental import pallas as pl
from jax.experimental.pallas import tpu as pltpu
from jax.sharding import PartitionSpec as P

MESH = pl.DeviceIdType.MESH


def half_slope(left, right):
    low = jnp.maximum(jnp.minimum(left, right), 0.0)
    high = jnp.minimum(jnp.maximum(left, right), 0.0)
    return jnp.maximum(jnp.minimum(0.25 * (left + right), low), high)


def chunks_of(fields, rows, group):
    rest = rows // group - 1
    if rest == 0:
        return [(True, f, 1) for f in range(fields)]
    return [(True, 0, fields), (False, 0, fields - 1), (False, fields - 1, 1)]


def peers_of(group, me):
    if group == 4:
        inner = me + 1 - 2 * lax.rem(me, 2)
        outer = lax.rem(me + 2, 4)
        return [inner, outer], [inner + outer - me]
    return [lax.rem(me + step, group) for step in range(1, group)], []


def kernel(
    group, rings, chunks,
    fields, shift_in, fraction_in, rates_in,
    out,
    own, landed, rate, bend, shift, fraction, rates, *rest,
):
    count = len(chunks)
    gathered, results = rest[:count], rest[count : 2 * count]
    small_sem, in_sem, own_sem, send1, recv1, send2, recv2, ghost_send, ghost_recv, passed = rest[2 * count :]
    nf, rows, polar, width = fields.shape
    me, ring = lax.axis_index("az"), lax.axis_index("rad")
    more = rows // group - 1
    start = ring * rows

    def base(first, d):
        if first:
            return jnp.where(d < 2, d, jnp.where(d < 4, rows - 4 + d, d - 2))
        return group - 2 + d * more

    def height(first):
        return 1 if first else more

    near, far = peers_of(group, me)
    barrier = pltpu.get_barrier_semaphore()
    for d in near:
        pl.semaphore_signal(barrier, inc=1, device_id=(d, ring), device_id_type=MESH)

    @pl.when(ring > 0)
    def _():
        pl.semaphore_signal(barrier, inc=1, device_id=(me, ring - 1), device_id_type=MESH)

    @pl.when(ring < rings - 1)
    def _():
        pl.semaphore_signal(barrier, inc=1, device_id=(me, ring + 1), device_id_type=MESH)

    stages = [
        pltpu.make_async_copy(fields.at[:, pl.ds(0, group - 2)], own.at[:, pl.ds(0, group - 2)], in_sem.at[0]),
        pltpu.make_async_copy(fields.at[:, pl.ds(rows - 2, 2)], own.at[:, pl.ds(rows - 2, 2)], in_sem.at[1]),
    ]
    if more:
        stages.append(
            pltpu.make_async_copy(
                fields.at[:, pl.ds(group - 2, rows - group)],
                own.at[:, pl.ds(group - 2, rows - group)],
                in_sem.at[2],
            )
        )
    for copy in stages:
        copy.start()
    mine = []
    for c, (first, f0, n) in enumerate(chunks):
        copy = pltpu.make_async_copy(
            fields.at[pl.ds(f0, n), pl.ds(base(first, me), height(first))],
            gathered[c].at[me],
            own_sem.at[c],
        )
        copy.start()
        mine.append(copy)

    small = [
        pltpu.make_async_copy(rates_in, rates, small_sem.at[0]),
        pltpu.make_async_copy(shift_in, shift, small_sem.at[1]),
        pltpu.make_async_copy(fraction_in, fraction, small_sem.at[2]),
    ]
    for copy in small:
        copy.start()

    neighbours = len(near) + jnp.where(ring > 0, 1, 0) + jnp.where(ring < rings - 1, 1, 0)
    pl.semaphore_wait(barrier, neighbours)
    if far:
        pl.semaphore_signal(passed, inc=1, device_id=(near[0], ring), device_id_type=MESH)

    def out_copy(c, d):
        first, f0, n = chunks[c]
        return pltpu.make_async_remote_copy(
            src_ref=own.at[pl.ds(f0, n), pl.ds(base(first, d), height(first))],
            dst_ref=gathered[c].at[me],
            send_sem=send1.at[c, d],
            recv_sem=recv1.at[c, me],
            device_id=(d, ring),
            device_id_type=MESH,
        )

    def in_copy(c, s):
        first, f0, n = chunks[c]
        return pltpu.make_async_remote_copy(
            src_ref=gathered[c].at[s],
            dst_ref=gathered[c].at[s],
            send_sem=send1.at[c, s],
            recv_sem=recv1.at[c, s],
            device_id=(s, ring),
            device_id_type=MESH,
        )

    def back_copy(c, d):
        first, f0, n = chunks[c]
        return pltpu.make_async_remote_copy(
            src_ref=results[c].at[d],
            dst_ref=landed.at[pl.ds(f0, n), pl.ds(2 + base(first, me), height(first))],
            send_sem=send2.at[c, d],
            recv_sem=recv2.at[c, me],
            device_id=(d, ring),
            device_id_type=MESH,
        )

    def home_copy(c, s):
        first, f0, n = chunks[c]
        target = landed.at[pl.ds(f0, n), pl.ds(2 + base(first, s), height(first))]
        return pltpu.make_async_remote_copy(
            src_ref=target,
            dst_ref=target,
            send_sem=send2.at[c, s],
            recv_sem=recv2.at[c, s],
            device_id=(s, ring),
            device_id_type=MESH,
        )

    def peers():
        return far + near

    for c in range(count):
        if c == 0:
            stages[0].wait()
            stages[1].wait()
        if c == 1 and more:
            stages[2].wait()
        for d in near if c == 0 else far + near:
            out_copy(c, d).start()
        if c == 0 and far:
            pl.semaphore_wait(passed, 1)
        for d in far if c == 0 else []:
            out_copy(c, d).start()

    small[0].wait()
    table = rates[...]
    place = lax.broadcasted_iota(jnp.int32, table.shape, 1)
    for j in range(rows + 1):
        column = jnp.sum(
            jnp.where(place == start - 1 + j, table, 0.0), axis=1, keepdims=True
        )
        if j == 0:
            column = jnp.where(ring > 0, column, 0.0)
        if j == rows:
            column = jnp.where(ring < rings - 1, column, 0.0)
        spread = jnp.broadcast_to(column, (polar, width))
        size = jnp.abs(spread)
        rate[j] = spread
        bend[j] = size * (1.0 - size)

    @pl.when(ring == 0)
    def _():
        landed[:, 0:2] = jnp.zeros((nf, 2, polar, width), jnp.float32)

    @pl.when(ring == rings - 1)
    def _():
        landed[:, rows + 2 : rows + 4] = jnp.zeros((nf, 2, polar, width), jnp.float32)

    lane = lax.broadcasted_iota(jnp.int32, (polar, width), 1)
    at_first, at_last = lane == 0, lane == width - 1

    def previous(blocks):
        turned = [pltpu.roll(b, 1, 1) for b in blocks]
        return [jnp.where(at_first, turned[p - 1], turned[p]) for p in range(group)]

    def following(blocks):
        turned = [pltpu.roll(b, width - 1, 1) for b in blocks]
        return [jnp.where(at_last, turned[(p + 1) % group], turned[p]) for p in range(group)]

    cycle = group * width

    def azimuth(c):
        first, f0, n = chunks[c]
        source, target = gathered[c], results[c]
        for k in range(height(first)):
            row = start + base(first, me) + k
            courant = fraction[row]
            ahead = courant > 0.0
            amount = shift[row] + jnp.where(ahead, cycle, cycle - 1)
            whole = lax.rem(amount // width, group)
            part = lax.rem(amount, width)
            size = jnp.abs(courant)
            bent = size * (1.0 - size)
            beyond = lane >= part

            for f in range(n):
                turned = [
                    pltpu.roll(source[lax.rem(p + group - whole, group), f, k], part, 1)
                    for p in range(group)
                ]
                q = [jnp.where(beyond, turned[p], turned[p - 1]) for p in range(group)]
                before = previous(q)
                left = [x - y for x, y in zip(q, before)]
                right = following(left)
                value = [
                    courant * x + bent * half_slope(l, r) for x, l, r in zip(q, left, right)
                ]
                lower = previous(value)
                for p in range(group):
                    kept = jnp.where(ahead, q[p], before[p])
                    target[p, f, k] = kept - (value[p] - lower[p])
        landed[pl.ds(f0, n), pl.ds(2 + base(first, me), height(first))] = target[me]

    ghosts = [
        pltpu.make_async_remote_copy(
            src_ref=landed.at[:, pl.ds(2, 2)],
            dst_ref=landed.at[:, pl.ds(rows + 2, 2)],
            send_sem=ghost_send.at[0],
            recv_sem=ghost_recv.at[0],
            device_id=(me, jnp.maximum(ring - 1, 0)),
            device_id_type=MESH,
        ),
        pltpu.make_async_remote_copy(
            src_ref=landed.at[:, pl.ds(rows, 2)],
            dst_ref=landed.at[:, pl.ds(0, 2)],
            send_sem=ghost_send.at[1],
            recv_sem=ghost_recv.at[1],
            device_id=(me, jnp.minimum(ring + 1, rings - 1)),
            device_id_type=MESH,
        ),
    ]

    def radial(f):
        def cell(i):
            return landed[f, i]

        q1, q2 = cell(1), cell(2)
        d1 = q1 - cell(0)
        d2 = q2 - q1
        h1 = half_slope(d1, d2)
        below = None
        for j in range(rows + 1):
            q3 = cell(j + 3)
            d3 = q3 - q2
            h2 = half_slope(d2, d3)
            c, b = rate[j], bend[j]
            ahead = c > 0.0
            flux = c * jnp.where(ahead, q1, q2) + b * jnp.where(ahead, h1, h2)
            if j > 0:
                out[f, j - 1] = q1 - (flux - below)
            below = flux
            q1, q2, d2, h1 = q2, q3, d3, h2

    edges = 1 if more else count

    small[1].wait()
    small[2].wait()
    for c in range(count):
        mine[c].wait()
        for s in peers():
            in_copy(c, s).wait_recv()
        azimuth(c)
        for d in peers():
            back_copy(c, d).start()

    for c in range(edges):
        for s in peers():
            home_copy(c, s).wait_recv()

    @pl.when(ring > 0)
    def _():
        ghosts[0].start()

    @pl.when(ring < rings - 1)
    def _():
        ghosts[1].start()

    @pl.when(ring > 0)
    def _():
        ghosts[1].wait_recv()

    @pl.when(ring < rings - 1)
    def _():
        ghosts[0].wait_recv()

    for c in range(edges, count):
        first, f0, n = chunks[c]
        for s in peers():
            home_copy(c, s).wait_recv()
        for f in range(f0, f0 + n):
            radial(f)
    if not more:
        for f in range(nf):
            radial(f)

    for c in range(count):
        for d in peers():
            out_copy(c, d).wait_send()
            back_copy(c, d).wait_send()

    @pl.when(ring > 0)
    def _():
        ghosts[0].wait_send()

    @pl.when(ring < rings - 1)
    def _():
        ghosts[1].wait_send()


def shards(fields, shift, fraction, radial_rate):
    nf, rows, polar, width = fields.shape
    group, rings = lax.axis_size("az"), lax.axis_size("rad")
    chunks = chunks_of(nf, rows, group)
    more = rows // group - 1
    boxes = [
        pltpu.VMEM((group, n, 1 if first else more, polar, width), jnp.float32)
        for first, f0, n in chunks
    ]
    count = len(chunks)
    dma = pltpu.SemaphoreType.DMA
    operands = (fields, shift, fraction, radial_rate.T)
    return pl.pallas_call(
        functools.partial(kernel, group, rings, chunks),
        out_shape=jax.ShapeDtypeStruct(fields.shape, jnp.float32),
        in_specs=[pl.BlockSpec(memory_space=pltpu.HBM)] * 4,
        out_specs=pl.BlockSpec(memory_space=pltpu.VMEM),
        scratch_shapes=[
            pltpu.VMEM((nf, rows, polar, width), jnp.float32),
            pltpu.VMEM((nf, rows + 4, polar, width), jnp.float32),
            pltpu.VMEM((rows + 1, polar, width), jnp.float32),
            pltpu.VMEM((rows + 1, polar, width), jnp.float32),
            pltpu.SMEM(shift.shape, jnp.int32),
            pltpu.SMEM(fraction.shape, jnp.float32),
            pltpu.VMEM(radial_rate.shape[::-1], jnp.float32),
            *boxes,
            *boxes,
            dma((3,)),
            dma((3,)),
            dma((count,)),
            dma((count, group)),
            dma((count, group)),
            dma((count, group)),
            dma((count, group)),
            dma((2,)),
            dma((2,)),
            pltpu.SemaphoreType.REGULAR,
        ],
        compiler_params=pltpu.CompilerParams(
            collective_id=0, has_side_effects=True, vmem_limit_bytes=10 * fields.size * 4
        ),
    )(*(pltpu.with_memory_space_constraint(x, pltpu.HBM) for x in operands))


def solution(mesh):
    placed = (P(None, "rad", None, "az"), P(), P(), P())
    return jax.shard_map(
        shards, mesh=mesh, in_specs=placed, out_specs=P(None, "rad", None, "az"), check_vma=False
    )
```

```python
import functools

import jax
import jax.numpy as jnp
from jax import lax
from jax.experimental import pallas as pl
from jax.experimental.pallas import tpu as pltpu
from jax.sharding import PartitionSpec as P

MESH = pl.DeviceIdType.MESH


def half_slope(left, right):
    low = jnp.maximum(jnp.minimum(left, right), 0.0)
    high = jnp.minimum(jnp.maximum(left, right), 0.0)
    return jnp.maximum(jnp.minimum(0.25 * (left + right), low), high)


def chunks_of(fields, rows, group):
    rest = rows // group - 1
    if rest == 0:
        return [(True, f, 1) for f in range(fields)]
    return [(True, 0, fields), (False, 0, fields - 2), (False, fields - 2, 2)]


def peers_of(group, me):
    if group == 4:
        inner = me + 1 - 2 * lax.rem(me, 2)
        outer = lax.rem(me + 2, 4)
        return [inner, outer], [inner + outer - me]
    return [lax.rem(me + step, group) for step in range(1, group)], []


def kernel(
    group, rings, chunks,
    fields, shift_in, fraction_in, rates_in,
    out,
    own, landed, rate, bend, shift, fraction, rates, *rest,
):
    count = len(chunks)
    gathered, results = rest[:count], rest[count : 2 * count]
    small_sem, in_sem, own_sem, send1, recv1, send2, recv2, ghost_send, ghost_recv, passed = rest[2 * count :]
    nf, rows, polar, width = fields.shape
    me, ring = lax.axis_index("az"), lax.axis_index("rad")
    more = rows // group - 1
    start = ring * rows

    def base(first, d):
        if first:
            return jnp.where(d < 2, d, jnp.where(d < 4, rows - 4 + d, d - 2))
        return group - 2 + d * more

    def height(first):
        return 1 if first else more

    near, far = peers_of(group, me)
    barrier = pltpu.get_barrier_semaphore()
    for d in near:
        pl.semaphore_signal(barrier, inc=1, device_id=(d, ring), device_id_type=MESH)

    @pl.when(ring > 0)
    def _():
        pl.semaphore_signal(barrier, inc=1, device_id=(me, ring - 1), device_id_type=MESH)

    @pl.when(ring < rings - 1)
    def _():
        pl.semaphore_signal(barrier, inc=1, device_id=(me, ring + 1), device_id_type=MESH)

    stages = [
        pltpu.make_async_copy(fields.at[:, pl.ds(0, group - 2)], own.at[:, pl.ds(0, group - 2)], in_sem.at[0]),
        pltpu.make_async_copy(fields.at[:, pl.ds(rows - 2, 2)], own.at[:, pl.ds(rows - 2, 2)], in_sem.at[1]),
    ]
    if more:
        stages.append(
            pltpu.make_async_copy(
                fields.at[:, pl.ds(group - 2, rows - group)],
                own.at[:, pl.ds(group - 2, rows - group)],
                in_sem.at[2],
            )
        )
    for copy in stages:
        copy.start()
    mine = []
    for c, (first, f0, n) in enumerate(chunks):
        copy = pltpu.make_async_copy(
            fields.at[pl.ds(f0, n), pl.ds(base(first, me), height(first))],
            gathered[c].at[me],
            own_sem.at[c],
        )
        copy.start()
        mine.append(copy)

    small = [
        pltpu.make_async_copy(rates_in, rates, small_sem.at[0]),
        pltpu.make_async_copy(shift_in, shift, small_sem.at[1]),
        pltpu.make_async_copy(fraction_in, fraction, small_sem.at[2]),
    ]
    for copy in small:
        copy.start()

    neighbours = len(near) + jnp.where(ring > 0, 1, 0) + jnp.where(ring < rings - 1, 1, 0)
    pl.semaphore_wait(barrier, neighbours)
    if far:
        pl.semaphore_signal(passed, inc=1, device_id=(near[0], ring), device_id_type=MESH)

    def out_copy(c, d):
        first, f0, n = chunks[c]
        return pltpu.make_async_remote_copy(
            src_ref=own.at[pl.ds(f0, n), pl.ds(base(first, d), height(first))],
            dst_ref=gathered[c].at[me],
            send_sem=send1.at[c, d],
            recv_sem=recv1.at[c, me],
            device_id=(d, ring),
            device_id_type=MESH,
        )

    def in_copy(c, s):
        first, f0, n = chunks[c]
        return pltpu.make_async_remote_copy(
            src_ref=gathered[c].at[s],
            dst_ref=gathered[c].at[s],
            send_sem=send1.at[c, s],
            recv_sem=recv1.at[c, s],
            device_id=(s, ring),
            device_id_type=MESH,
        )

    def back_copy(c, d):
        first, f0, n = chunks[c]
        return pltpu.make_async_remote_copy(
            src_ref=results[c].at[d],
            dst_ref=landed.at[pl.ds(f0, n), pl.ds(2 + base(first, me), height(first))],
            send_sem=send2.at[c, d],
            recv_sem=recv2.at[c, me],
            device_id=(d, ring),
            device_id_type=MESH,
        )

    def home_copy(c, s):
        first, f0, n = chunks[c]
        target = landed.at[pl.ds(f0, n), pl.ds(2 + base(first, s), height(first))]
        return pltpu.make_async_remote_copy(
            src_ref=target,
            dst_ref=target,
            send_sem=send2.at[c, s],
            recv_sem=recv2.at[c, s],
            device_id=(s, ring),
            device_id_type=MESH,
        )

    def peers():
        return far + near

    for c in range(count):
        if c == 0:
            stages[0].wait()
            stages[1].wait()
        if c == 1 and more:
            stages[2].wait()
        for d in near if c == 0 else far + near:
            out_copy(c, d).start()
        if c == 0 and far:
            pl.semaphore_wait(passed, 1)
        for d in far if c == 0 else []:
            out_copy(c, d).start()

    small[0].wait()
    table = rates[...]
    place = lax.broadcasted_iota(jnp.int32, table.shape, 1)
    for j in range(rows + 1):
        column = jnp.sum(
            jnp.where(place == start - 1 + j, table, 0.0), axis=1, keepdims=True
        )
        if j == 0:
            column = jnp.where(ring > 0, column, 0.0)
        if j == rows:
            column = jnp.where(ring < rings - 1, column, 0.0)
        spread = jnp.broadcast_to(column, (polar, width))
        size = jnp.abs(spread)
        rate[j] = spread
        bend[j] = size * (1.0 - size)

    @pl.when(ring == 0)
    def _():
        landed[:, 0:2] = jnp.zeros((nf, 2, polar, width), jnp.float32)

    @pl.when(ring == rings - 1)
    def _():
        landed[:, rows + 2 : rows + 4] = jnp.zeros((nf, 2, polar, width), jnp.float32)

    lane = lax.broadcasted_iota(jnp.int32, (polar, width), 1)
    at_first, at_last = lane == 0, lane == width - 1

    def previous(blocks):
        turned = [pltpu.roll(b, 1, 1) for b in blocks]
        return [jnp.where(at_first, turned[p - 1], turned[p]) for p in range(group)]

    def following(blocks):
        turned = [pltpu.roll(b, width - 1, 1) for b in blocks]
        return [jnp.where(at_last, turned[(p + 1) % group], turned[p]) for p in range(group)]

    cycle = group * width

    def azimuth(c):
        first, f0, n = chunks[c]
        source, target = gathered[c], results[c]
        for k in range(height(first)):
            row = start + base(first, me) + k
            courant = fraction[row]
            ahead = courant > 0.0
            amount = shift[row] + jnp.where(ahead, cycle, cycle - 1)
            whole = lax.rem(amount // width, group)
            part = lax.rem(amount, width)
            size = jnp.abs(courant)
            bent = size * (1.0 - size)
            beyond = lane >= part

            for f in range(n):
                turned = [
                    pltpu.roll(source[lax.rem(p + group - whole, group), f, k], part, 1)
                    for p in range(group)
                ]
                q = [jnp.where(beyond, turned[p], turned[p - 1]) for p in range(group)]
                before = previous(q)
                left = [x - y for x, y in zip(q, before)]
                right = following(left)
                value = [
                    courant * x + bent * half_slope(l, r) for x, l, r in zip(q, left, right)
                ]
                lower = previous(value)
                for p in range(group):
                    kept = jnp.where(ahead, q[p], before[p])
                    target[p, f, k] = kept - (value[p] - lower[p])
        landed[pl.ds(f0, n), pl.ds(2 + base(first, me), height(first))] = target[me]

    ghosts = [
        pltpu.make_async_remote_copy(
            src_ref=landed.at[:, pl.ds(2, 2)],
            dst_ref=landed.at[:, pl.ds(rows + 2, 2)],
            send_sem=ghost_send.at[0],
            recv_sem=ghost_recv.at[0],
            device_id=(me, jnp.maximum(ring - 1, 0)),
            device_id_type=MESH,
        ),
        pltpu.make_async_remote_copy(
            src_ref=landed.at[:, pl.ds(rows, 2)],
            dst_ref=landed.at[:, pl.ds(0, 2)],
            send_sem=ghost_send.at[1],
            recv_sem=ghost_recv.at[1],
            device_id=(me, jnp.minimum(ring + 1, rings - 1)),
            device_id_type=MESH,
        ),
    ]

    def radial(f):
        def cell(i):
            return landed[f, i]

        q1, q2 = cell(1), cell(2)
        d1 = q1 - cell(0)
        d2 = q2 - q1
        h1 = half_slope(d1, d2)
        below = None
        for j in range(rows + 1):
            q3 = cell(j + 3)
            d3 = q3 - q2
            h2 = half_slope(d2, d3)
            c, b = rate[j], bend[j]
            ahead = c > 0.0
            flux = c * jnp.where(ahead, q1, q2) + b * jnp.where(ahead, h1, h2)
            if j > 0:
                out[f, j - 1] = q1 - (flux - below)
            below = flux
            q1, q2, d2, h1 = q2, q3, d3, h2

    edges = 1 if more else count

    small[1].wait()
    small[2].wait()
    for c in range(count):
        mine[c].wait()
        for s in peers():
            in_copy(c, s).wait_recv()
        azimuth(c)
        for d in peers():
            back_copy(c, d).start()

    for c in range(edges):
        for s in peers():
            home_copy(c, s).wait_recv()

    @pl.when(ring > 0)
    def _():
        ghosts[0].start()

    @pl.when(ring < rings - 1)
    def _():
        ghosts[1].start()

    @pl.when(ring > 0)
    def _():
        ghosts[1].wait_recv()

    @pl.when(ring < rings - 1)
    def _():
        ghosts[0].wait_recv()

    for c in range(edges, count):
        first, f0, n = chunks[c]
        for s in peers():
            home_copy(c, s).wait_recv()
        for f in range(f0, f0 + n):
            radial(f)
    if not more:
        for f in range(nf):
            radial(f)

    for c in range(count):
        for d in peers():
            out_copy(c, d).wait_send()
            back_copy(c, d).wait_send()

    @pl.when(ring > 0)
    def _():
        ghosts[0].wait_send()

    @pl.when(ring < rings - 1)
    def _():
        ghosts[1].wait_send()


def shards(fields, shift, fraction, radial_rate):
    nf, rows, polar, width = fields.shape
    group, rings = lax.axis_size("az"), lax.axis_size("rad")
    chunks = chunks_of(nf, rows, group)
    more = rows // group - 1
    boxes = [
        pltpu.VMEM((group, n, 1 if first else more, polar, width), jnp.float32)
        for first, f0, n in chunks
    ]
    count = len(chunks)
    dma = pltpu.SemaphoreType.DMA
    operands = (fields, shift, fraction, radial_rate.T)
    return pl.pallas_call(
        functools.partial(kernel, group, rings, chunks),
        out_shape=jax.ShapeDtypeStruct(fields.shape, jnp.float32),
        in_specs=[pl.BlockSpec(memory_space=pltpu.HBM)] * 4,
        out_specs=pl.BlockSpec(memory_space=pltpu.VMEM),
        scratch_shapes=[
            pltpu.VMEM((nf, rows, polar, width), jnp.float32),
            pltpu.VMEM((nf, rows + 4, polar, width), jnp.float32),
            pltpu.VMEM((rows + 1, polar, width), jnp.float32),
            pltpu.VMEM((rows + 1, polar, width), jnp.float32),
            pltpu.SMEM(shift.shape, jnp.int32),
            pltpu.SMEM(fraction.shape, jnp.float32),
            pltpu.VMEM(radial_rate.shape[::-1], jnp.float32),
            *boxes,
            *boxes,
            dma((3,)),
            dma((3,)),
            dma((count,)),
            dma((count, group)),
            dma((count, group)),
            dma((count, group)),
            dma((count, group)),
            dma((2,)),
            dma((2,)),
            pltpu.SemaphoreType.REGULAR,
        ],
        compiler_params=pltpu.CompilerParams(
            collective_id=0, has_side_effects=True, vmem_limit_bytes=10 * fields.size * 4
        ),
    )(*(pltpu.with_memory_space_constraint(x, pltpu.HBM) for x in operands))


def solution(mesh):
    placed = (P(None, "rad", None, "az"), P(), P(), P())
    return jax.shard_map(
        shards, mesh=mesh, in_specs=placed, out_specs=P(None, "rad", None, "az"), check_vma=False
    )
```

```python
import functools

import jax
import jax.numpy as jnp
from jax import lax
from jax.experimental import pallas as pl
from jax.experimental.pallas import tpu as pltpu
from jax.sharding import PartitionSpec as P

MESH = pl.DeviceIdType.MESH


def half_slope(left, right):
    low = jnp.maximum(jnp.minimum(left, right), 0.0)
    high = jnp.minimum(jnp.maximum(left, right), 0.0)
    return jnp.maximum(jnp.minimum(0.25 * (left + right), low), high)


def chunks_of(fields, rows, group):
    rest = rows // group - 1
    if rest == 0:
        return [(True, f, 1) for f in range(fields)]
    return [(True, 0, fields), (False, 0, fields - 2), (False, fields - 2, 2)]


def peers_of(group, me):
    if group == 4:
        inner = me + 1 - 2 * lax.rem(me, 2)
        outer = lax.rem(me + 2, 4)
        return [inner, outer], [inner + outer - me]
    return [lax.rem(me + step, group) for step in range(1, group)], []


def kernel(
    group, rings, chunks,
    fields, shift_in, fraction_in, rates_in,
    out,
    own, landed, rate, bend, shift, fraction, rates, *rest,
):
    count = len(chunks)
    gathered, results = rest[:count], rest[count : 2 * count]
    small_sem, in_sem, own_sem, send1, recv1, send2, recv2, ghost_send, ghost_recv, passed = rest[2 * count :]
    nf, rows, polar, width = fields.shape
    me, ring = lax.axis_index("az"), lax.axis_index("rad")
    more = rows // group - 1
    start = ring * rows

    def base(first, d):
        if first:
            return jnp.where(d < 2, d, jnp.where(d < 4, rows - 4 + d, d - 2))
        return group - 2 + d * more

    def height(first):
        return 1 if first else more

    near, far = peers_of(group, me)
    barrier = pltpu.get_barrier_semaphore()
    for d in near:
        pl.semaphore_signal(barrier, inc=1, device_id=(d, ring), device_id_type=MESH)

    @pl.when(ring > 0)
    def _():
        pl.semaphore_signal(barrier, inc=1, device_id=(me, ring - 1), device_id_type=MESH)

    @pl.when(ring < rings - 1)
    def _():
        pl.semaphore_signal(barrier, inc=1, device_id=(me, ring + 1), device_id_type=MESH)

    stages = [
        pltpu.make_async_copy(fields.at[:, pl.ds(0, group - 2)], own.at[:, pl.ds(0, group - 2)], in_sem.at[0]),
        pltpu.make_async_copy(fields.at[:, pl.ds(rows - 2, 2)], own.at[:, pl.ds(rows - 2, 2)], in_sem.at[1]),
    ]
    if more:
        stages.append(
            pltpu.make_async_copy(
                fields.at[:, pl.ds(group - 2, rows - group)],
                own.at[:, pl.ds(group - 2, rows - group)],
                in_sem.at[2],
            )
        )
    for copy in stages:
        copy.start()
    mine = []
    for c, (first, f0, n) in enumerate(chunks):
        copy = pltpu.make_async_copy(
            fields.at[pl.ds(f0, n), pl.ds(base(first, me), height(first))],
            gathered[c].at[me],
            own_sem.at[c],
        )
        copy.start()
        mine.append(copy)

    small = [
        pltpu.make_async_copy(rates_in, rates, small_sem.at[0]),
        pltpu.make_async_copy(shift_in, shift, small_sem.at[1]),
        pltpu.make_async_copy(fraction_in, fraction, small_sem.at[2]),
    ]
    for copy in small:
        copy.start()

    neighbours = len(near) + jnp.where(ring > 0, 1, 0) + jnp.where(ring < rings - 1, 1, 0)
    pl.semaphore_wait(barrier, neighbours)
    if far:
        pl.semaphore_signal(passed, inc=1, device_id=(near[0], ring), device_id_type=MESH)

    def out_copy(c, d):
        first, f0, n = chunks[c]
        return pltpu.make_async_remote_copy(
            src_ref=own.at[pl.ds(f0, n), pl.ds(base(first, d), height(first))],
            dst_ref=gathered[c].at[me],
            send_sem=send1.at[c, d],
            recv_sem=recv1.at[c, me],
            device_id=(d, ring),
            device_id_type=MESH,
        )

    def in_copy(c, s):
        first, f0, n = chunks[c]
        return pltpu.make_async_remote_copy(
            src_ref=gathered[c].at[s],
            dst_ref=gathered[c].at[s],
            send_sem=send1.at[c, s],
            recv_sem=recv1.at[c, s],
            device_id=(s, ring),
            device_id_type=MESH,
        )

    def back_copy(c, d):
        first, f0, n = chunks[c]
        return pltpu.make_async_remote_copy(
            src_ref=results[c].at[d],
            dst_ref=landed.at[pl.ds(f0, n), pl.ds(2 + base(first, me), height(first))],
            send_sem=send2.at[c, d],
            recv_sem=recv2.at[c, me],
            device_id=(d, ring),
            device_id_type=MESH,
        )

    def home_copy(c, s):
        first, f0, n = chunks[c]
        target = landed.at[pl.ds(f0, n), pl.ds(2 + base(first, s), height(first))]
        return pltpu.make_async_remote_copy(
            src_ref=target,
            dst_ref=target,
            send_sem=send2.at[c, s],
            recv_sem=recv2.at[c, s],
            device_id=(s, ring),
            device_id_type=MESH,
        )

    def peers():
        return far + near

    def ready(c):
        if c == 0:
            stages[0].wait()
            stages[1].wait()
        if c == 1 and more:
            stages[2].wait()

    for c in range(min(2, count)):
        ready(c)
        for d in near:
            out_copy(c, d).start()
    if far:
        pl.semaphore_wait(passed, 1)
    for c in range(count):
        for d in far:
            out_copy(c, d).start()
        if c > 1:
            for d in near:
                out_copy(c, d).start()

    small[0].wait()
    table = rates[...]
    place = lax.broadcasted_iota(jnp.int32, table.shape, 1)
    for j in range(rows + 1):
        column = jnp.sum(
            jnp.where(place == start - 1 + j, table, 0.0), axis=1, keepdims=True
        )
        if j == 0:
            column = jnp.where(ring > 0, column, 0.0)
        if j == rows:
            column = jnp.where(ring < rings - 1, column, 0.0)
        spread = jnp.broadcast_to(column, (polar, width))
        size = jnp.abs(spread)
        rate[j] = spread
        bend[j] = size * (1.0 - size)

    @pl.when(ring == 0)
    def _():
        landed[:, 0:2] = jnp.zeros((nf, 2, polar, width), jnp.float32)

    @pl.when(ring == rings - 1)
    def _():
        landed[:, rows + 2 : rows + 4] = jnp.zeros((nf, 2, polar, width), jnp.float32)

    lane = lax.broadcasted_iota(jnp.int32, (polar, width), 1)
    at_first, at_last = lane == 0, lane == width - 1

    def previous(blocks):
        turned = [pltpu.roll(b, 1, 1) for b in blocks]
        return [jnp.where(at_first, turned[p - 1], turned[p]) for p in range(group)]

    def following(blocks):
        turned = [pltpu.roll(b, width - 1, 1) for b in blocks]
        return [jnp.where(at_last, turned[(p + 1) % group], turned[p]) for p in range(group)]

    cycle = group * width

    def azimuth(c):
        first, f0, n = chunks[c]
        source, target = gathered[c], results[c]
        for k in range(height(first)):
            row = start + base(first, me) + k
            courant = fraction[row]
            ahead = courant > 0.0
            amount = shift[row] + jnp.where(ahead, cycle, cycle - 1)
            whole = lax.rem(amount // width, group)
            part = lax.rem(amount, width)
            size = jnp.abs(courant)
            bent = size * (1.0 - size)
            beyond = lane >= part

            for f in range(n):
                turned = [
                    pltpu.roll(source[lax.rem(p + group - whole, group), f, k], part, 1)
                    for p in range(group)
                ]
                q = [jnp.where(beyond, turned[p], turned[p - 1]) for p in range(group)]
                before = previous(q)
                left = [x - y for x, y in zip(q, before)]
                right = following(left)
                value = [
                    courant * x + bent * half_slope(l, r) for x, l, r in zip(q, left, right)
                ]
                lower = previous(value)
                for p in range(group):
                    kept = jnp.where(ahead, q[p], before[p])
                    target[p, f, k] = kept - (value[p] - lower[p])
        landed[pl.ds(f0, n), pl.ds(2 + base(first, me), height(first))] = target[me]

    ghosts = [
        pltpu.make_async_remote_copy(
            src_ref=landed.at[:, pl.ds(2, 2)],
            dst_ref=landed.at[:, pl.ds(rows + 2, 2)],
            send_sem=ghost_send.at[0],
            recv_sem=ghost_recv.at[0],
            device_id=(me, jnp.maximum(ring - 1, 0)),
            device_id_type=MESH,
        ),
        pltpu.make_async_remote_copy(
            src_ref=landed.at[:, pl.ds(rows, 2)],
            dst_ref=landed.at[:, pl.ds(0, 2)],
            send_sem=ghost_send.at[1],
            recv_sem=ghost_recv.at[1],
            device_id=(me, jnp.minimum(ring + 1, rings - 1)),
            device_id_type=MESH,
        ),
    ]

    def radial(f):
        def cell(i):
            return landed[f, i]

        q1, q2 = cell(1), cell(2)
        d1 = q1 - cell(0)
        d2 = q2 - q1
        h1 = half_slope(d1, d2)
        below = None
        for j in range(rows + 1):
            q3 = cell(j + 3)
            d3 = q3 - q2
            h2 = half_slope(d2, d3)
            c, b = rate[j], bend[j]
            ahead = c > 0.0
            flux = c * jnp.where(ahead, q1, q2) + b * jnp.where(ahead, h1, h2)
            if j > 0:
                out[f, j - 1] = q1 - (flux - below)
            below = flux
            q1, q2, d2, h1 = q2, q3, d3, h2

    edges = 1 if more else count

    small[1].wait()
    small[2].wait()
    for c in range(count):
        mine[c].wait()
        for s in peers():
            in_copy(c, s).wait_recv()
        azimuth(c)
        for d in peers():
            back_copy(c, d).start()

    for c in range(edges):
        for s in peers():
            home_copy(c, s).wait_recv()

    @pl.when(ring > 0)
    def _():
        ghosts[0].start()

    @pl.when(ring < rings - 1)
    def _():
        ghosts[1].start()

    @pl.when(ring > 0)
    def _():
        ghosts[1].wait_recv()

    @pl.when(ring < rings - 1)
    def _():
        ghosts[0].wait_recv()

    for c in range(edges, count):
        first, f0, n = chunks[c]
        for s in peers():
            home_copy(c, s).wait_recv()
        for f in range(f0, f0 + n):
            radial(f)
    if not more:
        for f in range(nf):
            radial(f)

    for c in range(count):
        for d in peers():
            out_copy(c, d).wait_send()
            back_copy(c, d).wait_send()

    @pl.when(ring > 0)
    def _():
        ghosts[0].wait_send()

    @pl.when(ring < rings - 1)
    def _():
        ghosts[1].wait_send()


def shards(fields, shift, fraction, radial_rate):
    nf, rows, polar, width = fields.shape
    group, rings = lax.axis_size("az"), lax.axis_size("rad")
    chunks = chunks_of(nf, rows, group)
    more = rows // group - 1
    boxes = [
        pltpu.VMEM((group, n, 1 if first else more, polar, width), jnp.float32)
        for first, f0, n in chunks
    ]
    count = len(chunks)
    dma = pltpu.SemaphoreType.DMA
    operands = (fields, shift, fraction, radial_rate.T)
    return pl.pallas_call(
        functools.partial(kernel, group, rings, chunks),
        out_shape=jax.ShapeDtypeStruct(fields.shape, jnp.float32),
        in_specs=[pl.BlockSpec(memory_space=pltpu.HBM)] * 4,
        out_specs=pl.BlockSpec(memory_space=pltpu.VMEM),
        scratch_shapes=[
            pltpu.VMEM((nf, rows, polar, width), jnp.float32),
            pltpu.VMEM((nf, rows + 4, polar, width), jnp.float32),
            pltpu.VMEM((rows + 1, polar, width), jnp.float32),
            pltpu.VMEM((rows + 1, polar, width), jnp.float32),
            pltpu.SMEM(shift.shape, jnp.int32),
            pltpu.SMEM(fraction.shape, jnp.float32),
            pltpu.VMEM(radial_rate.shape[::-1], jnp.float32),
            *boxes,
            *boxes,
            dma((3,)),
            dma((3,)),
            dma((count,)),
            dma((count, group)),
            dma((count, group)),
            dma((count, group)),
            dma((count, group)),
            dma((2,)),
            dma((2,)),
            pltpu.SemaphoreType.REGULAR,
        ],
        compiler_params=pltpu.CompilerParams(
            collective_id=0, has_side_effects=True, vmem_limit_bytes=10 * fields.size * 4
        ),
    )(*(pltpu.with_memory_space_constraint(x, pltpu.HBM) for x in operands))


def solution(mesh):
    placed = (P(None, "rad", None, "az"), P(), P(), P())
    return jax.shard_map(
        shards, mesh=mesh, in_specs=placed, out_specs=P(None, "rad", None, "az"), check_vma=False
    )
```
